256 devices in a mesh: gx: 8 (over z_hi, x), gy: 4 (over z_lo), gz: 8 (over y, core).
Axes of the slice: x: 4, y: 4, z: 8 (z_hi: 2, z_lo: 4; z = z_hi * 4 + z_lo), core: 2. Of those that a mesh axis runs over, the one named last changes fastest.
Arguments:
- inputs: bfloat16 [2048, 6144], P(('gx', 'gz'), 'gy'), may hold values from -6 to 6
- norm_gain: float32 [6144], P('gy'), may hold values from 0.25 to 1.75
- norm_bias: float32 [6144], P('gy'), may hold values from -4 to 4
- pre_act: bfloat16 [2048, 24576], P(('gx', 'gy'), 'gz'), may hold values from -8 to 8
- grad_act: bfloat16 [2048, 24576], P(('gx', 'gy'), 'gz'), may hold values from -4 to 4
- up_weight: bfloat16 [8, 3072, 6144], P('gz', 'gx', 'gy'), may hold values from -0.078125 to 0.078125
Outputs:
- grad_inputs: bfloat16 [2048, 6144], P(('gx', 'gz'), 'gy')
- grad_gain: float32 [6144], P('gy')
- grad_bias: float32 [6144], P('gy')
- grad_weight: float32 [8, 3072, 6144], P('gz', 'gx', 'gy')
The draws below stay inside these ranges and needn't reach their ends.
All inputs are finite; a program needn't handle non-finite values.
Results may differ from the reference program's by a relative error of at most 0.0049.
Values may be sent and summed in bfloat16 or wider, within the bound.
No kernel may reach another device: no remote copies, remote signals or barrier semaphores. Data moves between devices by JAX's collectives and lax.ppermute only.
A program may use at most 64 MiB of HBM per device.

```python
import jax
import jax.numpy as jnp
from jax import lax

D = 6144
FF = 24576
TOKENS = 2048
FB = 3072
N_GZ = 8


def block_levels(stream_key, extent, pieces, low, top_value):
    gain, own = 1.0, jax.random.fold_in(stream_key, 6)
    for dim, parts in pieces:
        heights = jnp.exp(jax.random.uniform(jax.random.fold_in(own, dim), (parts,), jnp.float32, low / len(pieces), top_value / len(pieces)))
        gain = gain * jnp.repeat(heights, extent[dim] // parts).reshape([-1 if axis == dim else 1 for axis in range(len(extent))])
    return gain


def noise(own_key, extent, deviation, bound, shards=(), dtype=jnp.bfloat16):
    array = deviation * jax.random.normal(own_key, extent, jnp.float32)
    if shards:
        array = array * block_levels(own_key, extent, shards, -0.22, 0.18)
    return jnp.clip(array, -bound, bound).astype(dtype)


def setup_inputs(seed: int = 0) -> dict:
    seeds = jax.random.split(jax.random.key(seed), 7)
    return {
        "inputs": noise(seeds[0], (TOKENS, D), 1.0, 6.0, ((0, 64), (1, 4))),
        "norm_gain": jnp.clip(1.0 + 0.15 * jax.random.normal(seeds[1], (D,), jnp.float32), 0.25, 1.75),
        "norm_bias": noise(seeds[2], (D,), 0.7, 4.0, ((0, 4),), jnp.float32),
        "pre_act": noise(seeds[3], (TOKENS, FF), 1.5, 8.0, ((0, 32), (1, 8))),
        "grad_act": noise(seeds[4], (TOKENS, FF), 0.5, 4.0, ((0, 32), (1, 8))),
        "up_weight": noise(seeds[5], (N_GZ, FB, D), D ** -0.5, 0.078125, ((0, 8), (1, 8), (2, 4))),
    }


epsilon = 1e-05
root_half = 0.7071067811865476
gauss_norm = 0.3989422804014327

def reference(inputs, norm_gain, norm_bias, pre_act, grad_act, up_weight):
    widened = inputs.astype(jnp.float32)
    row_mean = lax.optimization_barrier(jnp.mean(widened, axis=1, keepdims=True))
    centred = widened - row_mean
    row_var = lax.optimization_barrier(jnp.mean(centred * centred, axis=1, keepdims=True))
    inv_std = lax.rsqrt(row_var + epsilon)
    x_hat = centred * inv_std
    normed = (x_hat * norm_gain + norm_bias).astype(jnp.bfloat16)
    pre_float = pre_act.astype(jnp.float32)
    slopes = 0.5 * (1.0 + jax.scipy.special.erf(pre_float * root_half)) + pre_float * jnp.exp(-0.5 * pre_float * pre_float) * gauss_norm
    grad_pre = (grad_act.astype(jnp.float32) * slopes).astype(jnp.bfloat16)
    weight = up_weight.reshape(FF, D)
    grad_normed = jnp.dot(grad_pre, weight, preferred_element_type=jnp.float32)
    grad_weight = lax.dot_general(grad_pre, normed, (((0,), (0,)), ((), ())), preferred_element_type=jnp.float32)
    grad_weight = grad_weight.reshape(N_GZ, FF // N_GZ, D)
    grad_gain = lax.optimization_barrier(jnp.sum(grad_normed * x_hat, axis=0))
    grad_bias = lax.optimization_barrier(jnp.sum(grad_normed, axis=0))
    scaled = grad_normed * norm_gain
    grad_inputs = inv_std * (scaled - lax.optimization_barrier(jnp.mean(scaled, axis=1, keepdims=True)) - x_hat * lax.optimization_barrier(jnp.mean(scaled * x_hat, axis=1, keepdims=True)))
    return (grad_inputs.astype(jnp.bfloat16), grad_gain, grad_bias, grad_weight)
```

```python
import jax
import jax.numpy as jnp
from jax import lax
from jax.experimental import pallas as pl
from jax.experimental.pallas import tpu as pltpu
from jax.sharding import Mesh
from jax.sharding import PartitionSpec as P

D = 6144
epsilon = 1e-05
root_half = 0.7071067811865476
gauss_norm = 0.3989422804014327
f32 = jnp.float32
bf16 = jnp.bfloat16

GX = ("zh", "x")
GZ = ("y", "core")
GX_GZ = GX + GZ
GX_GY = GX + ("gy",)


def shift(v, axis, by):
    n = lax.axis_size(axis)
    return lax.ppermute(v, axis, [(i, (i + by) % n) for i in range(n)])


def gather4(v, axis):
    return [v, shift(v, axis, 3), shift(v, axis, 2), shift(v, axis, 1)]


def scatter4(slots, axis):
    got = [shift(slots[s].astype(bf16), axis, s) for s in (1, 3, 2)]
    total = slots[0]
    for piece in got:
        total = total + piece.astype(f32)
    return total


def even_sum4(v, axis):
    a, b, c, d = gather4(v, axis)
    return (a + c) + (b + d)


def slope_kernel(at_ref, pre_ref, grad_ref, out_ref):
    zh, x, core = at_ref[0], at_ref[1], at_ref[2]
    width = out_ref.shape[-1]
    for far in range(2):
        for d in range(4):
            block = lax.rem(zh + far, 2) * 4 + lax.rem(x + d, 4)
            cols = pl.ds(pl.multiple_of(block * width, width), width)
            for half in range(2):
                rows = pl.ds(pl.multiple_of(lax.rem(core + half, 2) * 32, 32), 32)
                v = pre_ref[rows, cols].astype(f32)
                slope = 0.5 * (1.0 + lax.erf(v * root_half)) + v * jnp.exp(-0.5 * v * v) * gauss_norm
                out_ref[far, d, half] = (grad_ref[rows, cols].astype(f32) * slope).astype(bf16)


def grad_pre_blocks(pre_act, grad_act):
    at = jnp.stack([lax.axis_index("zh"), lax.axis_index("x"), lax.axis_index("core")])
    rows, cols = pre_act.shape
    return pl.pallas_call(
        slope_kernel,
        out_shape=jax.ShapeDtypeStruct((2, 4, 2, rows // 2, cols // 8), bf16),
        in_specs=[
            pl.BlockSpec(memory_space=pltpu.SMEM),
            pl.BlockSpec(memory_space=pltpu.VMEM),
            pl.BlockSpec(memory_space=pltpu.VMEM),
        ],
        out_specs=pl.BlockSpec(memory_space=pltpu.VMEM),
        cost_estimate=pl.CostEstimate(flops=20 * rows * cols, bytes_accessed=6 * rows * cols, transcendentals=2 * rows * cols),
    )(at, pre_act, grad_act)


def on_device(inputs, norm_gain, norm_bias, pre_act, grad_act, up_weight):
    weight = up_weight[0]
    hidden, width = weight.shape
    gy, y = lax.axis_index("gy"), lax.axis_index("y")

    blocks = grad_pre_blocks(pre_act, grad_act)
    mirror = [(4 * a + b, 4 * (1 - a) + 3 - b) for a in range(2) for b in range(4)]
    far = lax.ppermute(blocks[1], ("zh", "gy"), mirror)
    both = jnp.stack([blocks[0], far], axis=1)
    slots = [both[0]] + [None] * 3
    for d in (1, 3, 2):
        slots[(4 - d) % 4] = shift(both[d], "x", d)
    mine = jnp.stack(slots)

    up1 = lax.ppermute(mine, "gy", [(0, 1), (1, 2), (2, 3)])
    dn1 = lax.ppermute(mine, "gy", [(1, 0), (2, 1), (3, 2)])
    ends = lax.ppermute(mine, "gy", [(0, 3), (3, 0)])
    up2 = lax.ppermute(up1, "gy", [(1, 2), (2, 3)])
    dn2 = lax.ppermute(dn1, "gy", [(2, 1), (1, 0)])
    line = jnp.stack([ends, up2, up1, mine, dn1, dn2, ends])

    def rows_of(zr):
        parts = []
        for r in range(4):
            j = lax.rem(y + r, 4)
            at = (j if zr == 0 else 3 - j) - gy + 3
            part = lax.dynamic_slice(line, (at, 0, zr, 0, 0, 0), (1, 4, 1, 2, 32, hidden))
            parts.append(part.reshape(4, 2, 32, hidden))
        return jnp.stack(parts).transpose(2, 0, 1, 3, 4).reshape(2, 512, hidden)

    tokens = [rows_of(0), rows_of(1)]

    own = jnp.stack(gather4(jnp.stack(gather4(inputs, "x")), "y"))
    other = jnp.stack(gather4(jnp.stack(gather4(shift(inputs, "zh", 1), "y")), "x"), axis=1)
    raw = []
    for part in (own, other):
        part = part.reshape(512, width)
        raw.append(jnp.stack([part, shift(part, "core", 1)]))
    raw = jnp.stack(raw)
    widened = raw.astype(f32)
    sums = even_sum4(jnp.stack([jnp.sum(widened, axis=-1), jnp.sum(widened * widened, axis=-1)]), "gy")
    mean = sums[0] / D
    inv_std = lax.rsqrt(sums[1] / D - mean * mean + epsilon)
    x_hat = (widened - mean[..., None]) * inv_std[..., None]
    normed = (x_hat * norm_gain + norm_bias).astype(bf16)

    sums_over_tokens = []
    ends_at = []
    for zr in (1, 0):
        sent = jnp.dot(tokens[zr][1], weight, preferred_element_type=f32).astype(bf16)
        kept = jnp.dot(tokens[zr][0], weight, preferred_element_type=f32)
        chip = kept + shift(sent, "core", 1).astype(f32)
        sums_over_tokens.append(
            jnp.stack([jnp.sum(chip * x_hat[zr, 0], axis=0), jnp.sum(chip, axis=0)])
        )
        chip = chip.reshape(4, 4, 32, width)
        if zr == 0:
            line_sum = scatter4([chip[:, s] for s in range(4)], "x")
            ends_at.append(scatter4([line_sum[r] for r in range(4)], "y"))
        else:
            line_sum = scatter4([chip[r] for r in range(4)], "y")
            ends_at.append(scatter4([line_sum[s] for s in range(4)], "x"))
    grad_normed = ends_at[1] + shift(ends_at[0].astype(bf16), "zh", 1).astype(f32)

    grad_weight = lax.dot_general(
        jnp.stack(tokens).reshape(-1, hidden),
        normed.reshape(-1, width),
        (((0,), (0,)), ((), ())),
        preferred_element_type=f32,
    ).reshape(up_weight.shape)

    both_sums = sums_over_tokens[0] + sums_over_tokens[1]
    both_sums = both_sums + shift(both_sums, "core", 1)
    both_sums = even_sum4(both_sums, "y")
    both_sums = even_sum4(both_sums, "x")
    both_sums = both_sums + shift(both_sums, "zh", 1)

    own_hat = x_hat[0, 0, :32]
    own_std = inv_std[0, 0, :32, None]
    scaled = grad_normed * norm_gain
    row_sums = even_sum4(jnp.stack([jnp.sum(scaled, axis=1), jnp.sum(scaled * own_hat, axis=1)]), "gy")
    grad_inputs = own_std * (scaled - row_sums[0][:, None] / D - own_hat * (row_sums[1][:, None] / D))
    return (grad_inputs.astype(bf16), both_sums[0], both_sums[1], grad_weight)


def solution(mesh):
    split = Mesh(mesh.devices.reshape(2, 4, 4, 4, 2), ("zh", "x", "gy", "y", "core"))
    in_specs = (P(GX_GZ, "gy"), P("gy"), P("gy"), P(GX_GY, GZ), P(GX_GY, GZ), P(GZ, GX, "gy"))
    out_specs = (P(GX_GZ, "gy"), P("gy"), P("gy"), P(GZ, GX, "gy"))
    return jax.shard_map(
        on_device, mesh=split, in_specs=in_specs, out_specs=out_specs, check_vma=False
    )
```

```python
import jax
import jax.numpy as jnp
from jax import lax
from jax.experimental import pallas as pl
from jax.experimental.pallas import tpu as pltpu
from jax.sharding import Mesh
from jax.sharding import PartitionSpec as P


D = 6144
epsilon = 1e-05
root_half = 0.7071067811865476
gauss_norm = 0.3989422804014327
f32 = jnp.float32
bf16 = jnp.bfloat16

GX = ("zh", "x")
GZ = ("y", "core")
GX_GZ = GX + GZ
GX_GY = GX + ("gy",)


def swap(v, axis):
    return lax.ppermute(v, axis, [(0, 1), (1, 0)])


def exchange(v, axes):
    return lax.all_to_all(v, axes, 0, 0, tiled=True)


def shift(v, axis, by):
    return lax.ppermute(v, axis, [(i, (i + by) % 4) for i in range(4)])


def all_four(v, axis):
    at = lax.axis_index(axis)
    out = jnp.zeros((v.shape[0], 4, *v.shape[1:]), v.dtype)
    for by in range(4):
        block = shift(v, axis, by) if by else v
        out = lax.dynamic_update_index_in_dim(out, block, lax.rem(at + 4 - by, 4), 1)
    return out


def to_owners(v, axis):
    at = lax.axis_index(axis)
    total = lax.dynamic_index_in_dim(v, at, keepdims=False).astype(f32)
    for by in (1, 3, 2):
        block = lax.dynamic_index_in_dim(v, lax.rem(at + by, 4), keepdims=False)
        total = total + shift(block, axis, by).astype(f32)
    return total


def sum_of_four(v, axis):
    a, b, c, d = [v] + [shift(v, axis, by) for by in (1, 2, 3)]
    return (a + c) + (b + d)


def slope_kernel(core_ref, pre_ref, grad_ref, out_ref):
    core = core_ref[0]
    width = out_ref.shape[-1]

    @pl.loop(0, 8)
    def _(block):
        zh, x = block // 4, block % 4
        cols = pl.ds(pl.multiple_of(block * width, width), width)
        for half in range(2):
            rows = pl.ds(pl.multiple_of(lax.rem(core + half, 2) * 32, 32), 32)
            v = pre_ref[rows, cols].astype(f32)
            slope = 0.5 * (1.0 + lax.erf(v * root_half)) + v * jnp.exp(-0.5 * v * v) * gauss_norm
            value = (grad_ref[rows, cols].astype(f32) * slope).astype(bf16)
            for gy in range(4):
                out_ref[gy, x, zh, half] = value


def grad_pre_blocks(pre_act, grad_act):
    rows, cols = pre_act.shape
    return pl.pallas_call(
        slope_kernel,
        out_shape=jax.ShapeDtypeStruct((4, 4, 2, 2, rows // 2, cols // 8), bf16),
        in_specs=[
            pl.BlockSpec(memory_space=pltpu.SMEM),
            pl.BlockSpec(memory_space=pltpu.VMEM),
            pl.BlockSpec(memory_space=pltpu.VMEM),
        ],
        out_specs=pl.BlockSpec(memory_space=pltpu.VMEM),
        cost_estimate=pl.CostEstimate(flops=20 * rows * cols, bytes_accessed=12 * rows * cols, transcendentals=2 * rows * cols),
    )(lax.axis_index("core").reshape(1), pre_act, grad_act)


def on_device(inputs, norm_gain, norm_bias, pre_act, grad_act, up_weight):
    weight = up_weight[0]
    hidden, width = weight.shape
    zh, x, y = lax.axis_index("zh"), lax.axis_index("x"), lax.axis_index("y")

    far = swap(inputs, "zh")
    weights = weight, swap(weight, "core")
    blocks = grad_pre_blocks(pre_act, grad_act)
    blocks = exchange(blocks.reshape(32, 2, 32, hidden), ("gy", "x", "zh"))
    blocks = blocks.reshape(4, 4, 2, 2, 32, hidden)

    plane = all_four(jnp.stack([inputs, far]), "x").reshape(-1, width)
    planes = [plane] + [shift(plane, "y", by) for by in (3, 2, 1)]

    def two_zh(rows):
        return [lax.dynamic_index_in_dim(rows, (zh + k) % 2, 2, keepdims=False) for k in range(2)]

    mine, other = two_zh(blocks[:, :, :, 0]), two_zh(blocks[:, :, :, 1])
    given = two_zh(swap(blocks[:, :, :, 1], "core"))
    chip = []
    for k in range(2):
        a, b = mine[k], given[k]
        if k == 0:
            a, b = a.swapaxes(0, 1), b.swapaxes(0, 1)
        part = jnp.dot(a.reshape(512, hidden), weights[0], preferred_element_type=f32)
        part = part + jnp.dot(b.reshape(512, hidden), weights[1], preferred_element_type=f32)
        chip.append(part.astype(bf16).reshape(4, 4, 32, width))
    near = to_owners(to_owners(chip[0], "x").astype(bf16), "y")
    left = to_owners(to_owners(chip[1], "y").astype(bf16), "x")
    grad_normed = near + swap(left.astype(bf16), "zh").astype(f32)

    raw = [jnp.stack([v, swap(v, "core")]) for v in planes]
    sums = []
    for v in planes:
        v = v.astype(f32)
        sums.append(jnp.stack([jnp.sum(v, axis=-1), jnp.sum(v * v, axis=-1)]))
    sums = sum_of_four(jnp.stack(sums, axis=1), "gy")
    mean = sums[0] / D
    inv_std = lax.rsqrt(sums[1] / D - mean * mean + epsilon)
    mean, inv_std = jnp.stack([jnp.stack([mean, inv_std]), swap(jnp.stack([mean, inv_std]), "core")], axis=1)

    rows = jnp.stack([jnp.stack(v, axis=1) for v in (mine, other)], axis=1).reshape(4, 512, hidden)
    grad_weight = jnp.zeros((hidden, width), f32)
    both_sums = jnp.zeros((2, width), f32)
    for s, v in enumerate(raw):
        at = lax.rem(y + s, 4)
        x_hat = (v.astype(f32) - mean[:, s, :, None]) * inv_std[:, s, :, None]
        normed = (x_hat * norm_gain + norm_bias).astype(bf16)
        grad_weight = grad_weight + lax.dot_general(
            lax.dynamic_index_in_dim(rows, at, keepdims=False),
            normed.reshape(512, width),
            (((0,), (0,)), ((), ())),
            preferred_element_type=f32,
        )
        for k in range(2):
            part = lax.dynamic_index_in_dim(chip[k], at, 1 - k, keepdims=False)
            part = part.reshape(128, width).astype(f32)
            hat = x_hat[0, 128 * k : 128 * k + 128]
            both_sums = both_sums + jnp.stack([jnp.sum(part * hat, axis=0), jnp.sum(part, axis=0)])

    both_sums = both_sums + swap(both_sums, "core")
    both_sums = both_sums + swap(both_sums, "zh")
    both_sums = sum_of_four(sum_of_four(both_sums, "y"), "x")

    own = x * 32
    own_mean = lax.dynamic_slice_in_dim(mean[0, 0], own, 32)[:, None]
    own_std = lax.dynamic_slice_in_dim(inv_std[0, 0], own, 32)[:, None]
    own_hat = (inputs.astype(f32) - own_mean) * own_std
    scaled = grad_normed * norm_gain
    row_sums = jnp.stack([jnp.sum(scaled, axis=1), jnp.sum(scaled * own_hat, axis=1)])
    row_sums = sum_of_four(row_sums, "gy") / D
    grad_inputs = own_std * (scaled - row_sums[0][:, None] - own_hat * row_sums[1][:, None])
    return (grad_inputs.astype(bf16), both_sums[0], both_sums[1], grad_weight.reshape(up_weight.shape))


def solution(mesh):
    split = Mesh(mesh.devices.reshape(2, 4, 4, 4, 2), ("zh", "x", "gy", "y", "core"))
    in_specs = (P(GX_GZ, "gy"), P("gy"), P("gy"), P(GX_GY, GZ), P(GX_GY, GZ), P(GZ, GX, "gy"))
    out_specs = (P(GX_GZ, "gy"), P("gy"), P("gy"), P(GZ, GX, "gy"))

    return jax.shard_map(on_device, mesh=split, in_specs=in_specs, out_specs=out_specs, check_vma=False)
```

```python
import jax
import jax.numpy as jnp
from jax import lax
from jax.experimental import pallas as pl
from jax.experimental.pallas import tpu as pltpu
from jax.sharding import Mesh
from jax.sharding import PartitionSpec as P


D = 6144
epsilon = 1e-05
root_half = 0.7071067811865476
gauss_norm = 0.3989422804014327
f32 = jnp.float32
bf16 = jnp.bfloat16

GX = ("zh", "x")
GZ = ("y", "core")
GX_GZ = GX + GZ
GX_GY = GX + ("gy",)


def swap(v, axis):
    return lax.ppermute(v, axis, [(0, 1), (1, 0)])


def exchange(v, axes):
    return lax.all_to_all(v, axes, 0, 0, tiled=True)


def shift(v, axis, by):
    return lax.ppermute(v, axis, [(i, (i + by) % 4) for i in range(4)])


def all_four(v, axis):
    at = lax.axis_index(axis)
    out = jnp.zeros((v.shape[0], 4, *v.shape[1:]), v.dtype)
    for by in range(4):
        block = shift(v, axis, by) if by else v
        out = lax.dynamic_update_index_in_dim(out, block, lax.rem(at + 4 - by, 4), 1)
    return out


def to_owners(v, axis):
    at = lax.axis_index(axis)
    total = lax.dynamic_index_in_dim(v, at, keepdims=False).astype(f32)
    for by in (1, 3, 2):
        block = lax.dynamic_index_in_dim(v, lax.rem(at + by, 4), keepdims=False)
        total = total + shift(block, axis, by).astype(f32)
    return total


def group_sum(v, axes):
    n = lax.axis_size(axes)
    return jnp.sum(exchange(jnp.broadcast_to(v[None], (n, *v.shape)), axes), axis=0)


def slope_kernel(core_ref, pre_ref, grad_ref, out_ref):
    core = core_ref[0]
    width = out_ref.shape[-1]

    @pl.loop(0, 8)
    def _(block):
        zh, x = block // 4, block % 4
        cols = pl.ds(pl.multiple_of(block * width, width), width)
        for half in range(2):
            rows = pl.ds(pl.multiple_of(lax.rem(core + half, 2) * 32, 32), 32)
            v = pre_ref[rows, cols].astype(f32)
            slope = 0.5 * (1.0 + lax.erf(v * root_half)) + v * jnp.exp(-0.5 * v * v) * gauss_norm
            value = (grad_ref[rows, cols].astype(f32) * slope).astype(bf16)
            for gy in range(4):
                out_ref[gy, x, zh, half] = value


def grad_pre_blocks(pre_act, grad_act):
    rows, cols = pre_act.shape
    return pl.pallas_call(
        slope_kernel,
        out_shape=jax.ShapeDtypeStruct((4, 4, 2, 2, rows // 2, cols // 8), bf16),
        in_specs=[
            pl.BlockSpec(memory_space=pltpu.SMEM),
            pl.BlockSpec(memory_space=pltpu.VMEM),
            pl.BlockSpec(memory_space=pltpu.VMEM),
        ],
        out_specs=pl.BlockSpec(memory_space=pltpu.VMEM),
        cost_estimate=pl.CostEstimate(flops=20 * rows * cols, bytes_accessed=12 * rows * cols, transcendentals=2 * rows * cols),
    )(lax.axis_index("core").reshape(1), pre_act, grad_act)


def on_device(inputs, norm_gain, norm_bias, pre_act, grad_act, up_weight):
    weight = up_weight[0]
    hidden, width = weight.shape
    zh, x, y = lax.axis_index("zh"), lax.axis_index("x"), lax.axis_index("y")

    far = swap(inputs, "zh")
    weights = weight, swap(weight, "core")
    blocks = grad_pre_blocks(pre_act, grad_act)
    blocks = exchange(blocks.reshape(32, 2, 32, hidden), ("gy", "x", "zh"))
    blocks = blocks.reshape(4, 4, 2, 2, 32, hidden)

    plane = all_four(jnp.stack([inputs, far]), "x").reshape(-1, width)
    planes = [plane] + [shift(plane, "y", by) for by in (3, 2, 1)]

    def two_zh(rows):
        return [lax.dynamic_index_in_dim(rows, (zh + k) % 2, 2, keepdims=False) for k in range(2)]

    mine, other = two_zh(blocks[:, :, :, 0]), two_zh(blocks[:, :, :, 1])
    given = two_zh(swap(blocks[:, :, :, 1], "core"))
    chip = []
    for k in range(2):
        a, b = mine[k], given[k]
        if k == 0:
            a, b = a.swapaxes(0, 1), b.swapaxes(0, 1)
        part = jnp.dot(a.reshape(512, hidden), weights[0], preferred_element_type=f32)
        part = part + jnp.dot(b.reshape(512, hidden), weights[1], preferred_element_type=f32)
        chip.append(part.astype(bf16).reshape(4, 4, 32, width))
    near = to_owners(to_owners(chip[0], "x").astype(bf16), "y")
    left = to_owners(to_owners(chip[1], "y").astype(bf16), "x")
    grad_normed = near + swap(left.astype(bf16), "zh").astype(f32)

    raw = [jnp.stack([v, swap(v, "core")]) for v in planes]
    sums = []
    for v in planes:
        v = v.astype(f32)
        sums.append(jnp.stack([jnp.sum(v, axis=-1), jnp.sum(v * v, axis=-1)]))
    sums = group_sum(jnp.stack(sums, axis=1), "gy")
    mean = sums[0] / D
    inv_std = lax.rsqrt(sums[1] / D - mean * mean + epsilon)
    mean, inv_std = jnp.stack([jnp.stack([mean, inv_std]), swap(jnp.stack([mean, inv_std]), "core")], axis=1)

    rows = jnp.stack([jnp.stack(v, axis=1) for v in (mine, other)], axis=1).reshape(4, 512, hidden)
    grad_weight = jnp.zeros((hidden, width), f32)
    both_sums = jnp.zeros((2, width), f32)
    for s, v in enumerate(raw):
        at = lax.rem(y + s, 4)
        x_hat = (v.astype(f32) - mean[:, s, :, None]) * inv_std[:, s, :, None]
        normed = (x_hat * norm_gain + norm_bias).astype(bf16)
        grad_weight = grad_weight + lax.dot_general(
            lax.dynamic_index_in_dim(rows, at, keepdims=False),
            normed.reshape(512, width),
            (((0,), (0,)), ((), ())),
            preferred_element_type=f32,
        )
        for k in range(2):
            part = lax.dynamic_index_in_dim(chip[k], at, 1 - k, keepdims=False)
            part = part.reshape(128, width).astype(f32)
            hat = x_hat[0, 128 * k : 128 * k + 128]
            both_sums = both_sums + jnp.stack([jnp.sum(part * hat, axis=0), jnp.sum(part, axis=0)])

    both_sums = both_sums + swap(both_sums, "core")
    both_sums = both_sums + swap(both_sums, "zh")
    both_sums = group_sum(both_sums, ("y", "x"))

    own = x * 32
    own_mean = lax.dynamic_slice_in_dim(mean[0, 0], own, 32)[:, None]
    own_std = lax.dynamic_slice_in_dim(inv_std[0, 0], own, 32)[:, None]
    own_hat = (inputs.astype(f32) - own_mean) * own_std
    scaled = grad_normed * norm_gain
    row_sums = jnp.stack([jnp.sum(scaled, axis=1), jnp.sum(scaled * own_hat, axis=1)])
    row_sums = group_sum(row_sums, "gy") / D
    grad_inputs = own_std * (scaled - row_sums[0][:, None] - own_hat * row_sums[1][:, None])
    return (grad_inputs.astype(bf16), both_sums[0], both_sums[1], grad_weight.reshape(up_weight.shape))


def solution(mesh):
    split = Mesh(mesh.devices.reshape(2, 4, 4, 4, 2), ("zh", "x", "gy", "y", "core"))
    in_specs = (P(GX_GZ, "gy"), P("gy"), P("gy"), P(GX_GY, GZ), P(GX_GY, GZ), P(GZ, GX, "gy"))
    out_specs = (P(GX_GZ, "gy"), P("gy"), P("gy"), P(GZ, GX, "gy"))

    return jax.shard_map(on_device, mesh=split, in_specs=in_specs, out_specs=out_specs, check_vma=False)
```
